256 devices in a mesh: row: 32 (over x_lo, z, core), col: 8 (over x_hi, y).
Axes of the slice: x: 4 (x_hi: 2, x_lo: 2; x = x_hi * 2 + x_lo), y: 4, z: 8, core: 2. Of those that a mesh axis runs over, the one named last changes fastest.
Arguments:
- joined: bfloat16 [2, 32, 32, 28, 4096], P(None, None, 'row', None, 'col'), may hold values from -0.09375 to 0.09375
- probes: bfloat16 [2, 128, 4096], P(None, None, 'col'), may hold values from -6 to 6
Outputs:
- gate_rows: bfloat16 [2, 14336, 4096], P(None, 'row', 'col')
- up_rows: bfloat16 [2, 14336, 4096], P(None, 'row', 'col')
- hidden: bfloat16 [2, 128, 14336], P(None, 'col', 'row')
The draws below stay inside these ranges and needn't reach their ends.
All inputs are finite; a program needn't handle non-finite values.
Results may differ from the reference program's by a relative error of at most 0.002.
Values may be sent and summed in bfloat16 or wider, within the bound.
A program may use at most 64 MiB of HBM per device.

```python
import jax
import jax.numpy as jnp

D = 4096
FF = 14336
HALF = 14
LAYERS = 2
TOKENS = 128
CYCLES = 32
N_ROW = 32


def block_levels(rng, dims, split, least, largest):
    factor_of = 1.0
    for dim, blocks in split:
        heights = jax.random.uniform(jax.random.fold_in(jax.random.fold_in(rng, 6), dim), (blocks,), jnp.float32, least / len(split), largest / len(split))
        factor_of = factor_of * jnp.repeat(jnp.exp(heights), dims[dim] // blocks).reshape((-1,) + (1,) * (len(dims) - 1 - dim))
    return factor_of


def gaussian(rng, extent, deviation, reach, split=(), held_as=jnp.bfloat16):
    values = deviation * jax.random.normal(rng, extent, jnp.float32)
    if split:
        values = values * block_levels(rng, extent, split, -0.22, 0.18)
    return jnp.clip(values, -reach, reach).astype(held_as)


def setup_inputs(seed: int = 0) -> dict:
    splits = jax.random.split(jax.random.key(seed), 3)
    return {
        "joined": gaussian(splits[0], (LAYERS, CYCLES, N_ROW, 2 * HALF, D), D ** -0.5, 0.09375, ((2, 32), (4, 8))),
        "probes": gaussian(splits[1], (LAYERS, TOKENS, D), 1.0, 6.0, ((2, 8),)),
    }


def reference(joined, probes):
    blocks = joined.reshape(LAYERS, CYCLES * N_ROW, HALF, 2, D)
    gate_rows = blocks[:, :, :, 0, :].reshape(LAYERS, FF, D)
    up_rows = blocks[:, :, :, 1, :].reshape(LAYERS, FF, D)
    results = []
    for layer_index in range(LAYERS):
        gate_proj = jnp.dot(probes[layer_index], gate_rows[layer_index].T, preferred_element_type=jnp.float32)
        up_proj = jnp.dot(probes[layer_index], up_rows[layer_index].T, preferred_element_type=jnp.float32)
        results.append((jax.nn.silu(gate_proj) * up_proj).astype(jnp.bfloat16))
    hidden = jnp.stack(results, axis=0)
    return gate_rows, up_rows, hidden
```

```python
import functools

import jax
import jax.numpy as jnp
from jax import lax
from jax.experimental import pallas as pl
from jax.experimental.pallas import tpu as pltpu
from jax.sharding import PartitionSpec as P

MESH = pl.DeviceIdType.MESH
L, C, R, B, W = 2, 32, 32, 28, 512
HB = B // 2
J = L * B
T = 128
NY, NX = 4, 2
TC = T // (NY * NX)
PITCH = C + 1
LANES = 128
TILES = W // LANES
HALFW = 512
ROWS = C * HB


def exchange(
    x_hbm, p_hbm, got, hid, xs, pv, spread, msg, part, in_a, summed, in_b, hidt, hsend, hgot, order,
    load_sem, p_sem, own_sem, w_send, w_recv, a_send, a_recv, b_send, b_recv, h_send, h_recv,
):
    me = lax.axis_index("row")
    col = lax.axis_index("col")
    xh, y = col // NY, col % NY

    for gu in range(2):
        for l in range(L):
            q = gu * L + l
            pltpu.make_async_copy(x_hbm.at[l, :, gu], xs.at[pl.ds(q * HB, HB)], load_sem.at[q]).start()
    pltpu.make_async_copy(p_hbm, pv, p_sem).start()

    barrier = pltpu.get_barrier_semaphore()

    def hello(i, _):
        pl.semaphore_signal(barrier, inc=1, device_id={"row": (me + i) % R}, device_id_type=MESH)
        return _

    lax.fori_loop(1, R, hello, 0)
    for dy in range(1, NY):
        pl.semaphore_signal(barrier, inc=1, device_id={"col": xh * NY + (y + dy) % NY}, device_id_type=MESH)
    partner = (1 - xh) * NY + y
    pl.semaphore_signal(barrier, inc=1, device_id={"col": partner}, device_id_type=MESH)

    for q in range(2 * L):
        pltpu.make_async_copy(x_hbm.at[q % L, :, q // L], xs.at[pl.ds(q * HB, HB)], load_sem.at[q]).wait()
        for i in range(HB):
            j = q * HB + i
            rows = xs[j].astype(jnp.float32)
            for c in range(TILES):
                spread[c, pl.ds(j * PITCH, C), :] = rows[:, c * LANES:(c + 1) * LANES]
    for k in range(C):
        for c in range(TILES):
            msg[k, :, pl.ds(c * LANES, LANES)] = spread[c, pl.ds(k, J, stride=PITCH), :].astype(jnp.bfloat16)

    pltpu.make_async_copy(p_hbm, pv, p_sem).wait()
    for l in range(L):
        for gu in range(2):
            rows = xs[pl.ds((gu * L + l) * HB, HB)].reshape(ROWS, W)
            proj = lax.dot_general(
                pv[l], rows, (((1,), (1,)), ((), ())), preferred_element_type=jnp.float32
            )
            for a in range(NX):
                for b in range(NY):
                    t = (a * NY + b) * TC
                    part[b, a, l, :, pl.ds(gu * HALFW, ROWS)] = proj[t:t + TC]

    pl.semaphore_wait(barrier, R - 1 + NY)

    def weights(i):
        to = (me + i) % R
        return pltpu.make_async_remote_copy(
            src_ref=msg.at[to], dst_ref=got.at[me], send_sem=w_send.at[i], recv_sem=w_recv.at[me],
            device_id={"row": to}, device_id_type=MESH,
        )

    def hiddens(i):
        to = (me + i) % R
        return pltpu.make_async_remote_copy(
            src_ref=hsend.at[to], dst_ref=hgot.at[me], send_sem=h_send.at[i], recv_sem=h_recv.at[me],
            device_id={"row": to}, device_id_type=MESH,
        )

    def start_weights(i, _):
        weights(i).start()
        return _

    def phase_a(dy):
        to = (y + dy) % NY
        return pltpu.make_async_remote_copy(
            src_ref=part.at[to], dst_ref=in_a.at[dy - 1], send_sem=a_send.at[dy - 1], recv_sem=a_recv.at[dy - 1],
            device_id={"col": xh * NY + to}, device_id_type=MESH,
        )

    for dy in range(1, NY):
        phase_a(dy).start()
    lax.fori_loop(1, R, start_weights, 0)
    own = pltpu.make_async_copy(msg.at[me], got.at[me], own_sem)
    own.start()

    for dy in range(1, NY):
        phase_a(dy).wait()
    summed[...] = part[y] + in_a[0] + in_a[1] + in_a[2]
    phase_b = pltpu.make_async_remote_copy(
        src_ref=summed.at[1 - xh], dst_ref=in_b, send_sem=b_send, recv_sem=b_recv,
        device_id={"col": partner}, device_id_type=MESH,
    )
    phase_b.start()
    phase_b.wait()
    total = summed[xh] + in_b[...]
    gate, up = total[:, :, :HALFW], total[:, :, HALFW:]
    act = gate / (1.0 + jnp.exp(-gate)) * up
    stacked = jnp.concatenate(
        [act[l, :, g * LANES:(g + 1) * LANES] for g in range(4) for l in range(L)], axis=0
    )
    hidt[...] = stacked.T
    for k in range(C):
        hsend[k] = hidt[pl.ds(k, 4, stride=C), :].astype(jnp.bfloat16)

    def start_hidden(i, _):
        hiddens(i).start()
        return _

    lax.fori_loop(1, R, start_hidden, 0)
    hgot[me] = hsend[me]

    def wait_hidden(i, _):
        src = (me + i) % R
        pltpu.make_async_copy(hsend.at[0], hgot.at[src], h_recv.at[src]).wait()
        return _

    for i in range(1, R):
        hiddens(i).wait_send()
    for i in range(1, R):
        src = (me + i) % R
        pltpu.make_async_remote_copy(
            src_ref=hsend.at[0], dst_ref=hgot.at[src], send_sem=h_send.at[i], recv_sem=h_recv.at[src],
            device_id={"row": src}, device_id_type=MESH,
        ).wait_recv()
    for g in (3, 0, 1, 2):
        n = 2 if g == 3 else 4
        for p in range(R):
            piece = hgot[p].astype(jnp.float32)
            order[pl.ds(p * HB + 4 * g, n), :] = pltpu.roll(piece, (LANES - 32 * g) % LANES, 1)[:n]
    flat = order[...].T
    for l in range(L):
        hid[l] = flat[l * TC:(l + 1) * TC, :ROWS].astype(jnp.bfloat16)

    own.wait()
    for i in range(1, R):
        src = (me + i) % R
        weights(i).wait_send()
        pltpu.make_async_remote_copy(
            src_ref=msg.at[0], dst_ref=got.at[src], send_sem=w_send.at[i], recv_sem=w_recv.at[src],
            device_id={"row": src}, device_id_type=MESH,
        ).wait_recv()


def arrange(got, hid_in, gate, up, hid, flat, lined):
    flat[...] = got[...].astype(jnp.float32).reshape(R * J, LANES)
    for p in range(R):
        for q in range(2 * L):
            lined[q, pl.ds(p * HB, HB), :] = flat[pl.ds(p * J + q * HB, HB), :]
    for l in range(L):
        gate[l] = lined[l].astype(jnp.bfloat16)
        up[l] = lined[L + l].astype(jnp.bfloat16)
    hid[...] = hid_in[...]


def body(joined, probes):
    x = jnp.transpose(joined, (0, 2, 3, 1, 4)).reshape(L, HB, 2, C, W)
    anywhere = pl.BlockSpec(memory_space=pl.ANY)
    dma = pltpu.SemaphoreType.DMA
    f32, bf16 = jnp.float32, jnp.bfloat16
    got, hid = pl.pallas_call(
        exchange,
        out_shape=(
            jax.ShapeDtypeStruct((R, J, W), bf16),
            jax.ShapeDtypeStruct((L, TC, ROWS), bf16),
        ),
        in_specs=[anywhere, anywhere],
        out_specs=(anywhere, pl.BlockSpec(memory_space=pltpu.VMEM)),
        scratch_shapes=[
            pltpu.VMEM((J, C, W), bf16),
            pltpu.VMEM((L, T, W), bf16),
            pltpu.VMEM((TILES, J * PITCH, LANES), f32),
            pltpu.VMEM((C, J, W), bf16),
            pltpu.VMEM((NY, NX, L, TC, 2 * HALFW), f32),
            pltpu.VMEM((NY - 1, NX, L, TC, 2 * HALFW), f32),
            pltpu.VMEM((NX, L, TC, 2 * HALFW), f32),
            pltpu.VMEM((L, TC, 2 * HALFW), f32),
            pltpu.VMEM((LANES, LANES), f32),
            pltpu.VMEM((C, 4, LANES), bf16),
            pltpu.VMEM((R, 4, LANES), bf16),
            pltpu.VMEM((512, LANES), f32),
            dma((2 * L,)), dma, dma,
            dma((R,)), dma((R,)),
            dma((NY - 1,)), dma((NY - 1,)),
            dma, dma,
            dma((R,)), dma((R,)),
        ],
        compiler_params=pltpu.CompilerParams(
            collective_id=0, has_side_effects=True, vmem_limit_bytes=32 * 2**20
        ),
        name="exchange",
    )(x, probes)
    gate, up, hidden = pl.pallas_call(
        arrange,
        grid=(TILES,),
        out_shape=(
            jax.ShapeDtypeStruct((L, ROWS, W), bf16),
            jax.ShapeDtypeStruct((L, ROWS, W), bf16),
            jax.ShapeDtypeStruct((L, TC, ROWS), bf16),
        ),
        in_specs=[
            pl.BlockSpec((R, J, LANES), lambda c: (0, 0, c)),
            pl.BlockSpec((L, TC, ROWS), lambda c: (0, 0, 0)),
        ],
        out_specs=(
            pl.BlockSpec((L, ROWS, LANES), lambda c: (0, 0, c)),
            pl.BlockSpec((L, ROWS, LANES), lambda c: (0, 0, c)),
            pl.BlockSpec((L, TC, ROWS), lambda c: (0, 0, 0)),
        ),
        scratch_shapes=[
            pltpu.VMEM((R * J, LANES), f32),
            pltpu.VMEM((2 * L, ROWS, LANES), f32),
        ],
        name="arrange",
    )(got, hid)
    return gate, up, hidden


def solution(mesh):
    return jax.shard_map(
        body,
        mesh=mesh,
        in_specs=(P(None, None, "row", None, "col"), P(None, None, "col")),
        out_specs=(P(None, "row", "col"), P(None, "row", "col"), P(None, "col", "row")),
        check_vma=False,
    )
```

```python
import functools

import jax
import jax.numpy as jnp
from jax import lax
from jax.experimental import pallas as pl
from jax.experimental.pallas import tpu as pltpu
from jax.sharding import PartitionSpec as P

MESH = pl.DeviceIdType.MESH
L, C, R, B, W = 2, 32, 32, 28, 512
HB = B // 2
J = L * B
T = 128
NY, NX = 4, 2
TC = T // (NY * NX)
PITCH = C + 1
LANES = 128
TILES = W // LANES
HALFW = 512
ROWS = C * HB


def exchange(
    x_hbm, p_hbm, gate, up, hid, xs, pv, spread, msg, got, stage, lined, part, in_a, summed, in_b, hidt, hsend, hgot, order,
    load_sem, p_sem, w_send, w_recv, a_send, a_recv, b_send, b_recv, h_send, h_recv,
):
    me = lax.axis_index("row")
    col = lax.axis_index("col")
    xh, y = col // NY, col % NY

    for gu in range(2):
        for l in range(L):
            q = gu * L + l
            pltpu.make_async_copy(x_hbm.at[l, :, gu], xs.at[pl.ds(q * HB, HB)], load_sem.at[q]).start()
    pltpu.make_async_copy(p_hbm, pv, p_sem).start()

    barrier = pltpu.get_barrier_semaphore()

    def hello(i, _):
        pl.semaphore_signal(barrier, inc=1, device_id={"row": (me + i) % R}, device_id_type=MESH)
        return _

    lax.fori_loop(1, R, hello, 0)
    for dy in range(1, NY):
        pl.semaphore_signal(barrier, inc=1, device_id={"col": xh * NY + (y + dy) % NY}, device_id_type=MESH)
    partner = (1 - xh) * NY + y
    pl.semaphore_signal(barrier, inc=1, device_id={"col": partner}, device_id_type=MESH)

    for q in range(2 * L):
        pltpu.make_async_copy(x_hbm.at[q % L, :, q // L], xs.at[pl.ds(q * HB, HB)], load_sem.at[q]).wait()
        for i in range(HB):
            j = q * HB + i
            rows = xs[j].astype(jnp.float32)
            for c in range(TILES):
                spread[c, pl.ds(j * PITCH, C), :] = rows[:, c * LANES:(c + 1) * LANES]
    for k in range(C):
        for c in range(TILES):
            msg[k, :, pl.ds(c * LANES, LANES)] = spread[c, pl.ds(k, J, stride=PITCH), :].astype(jnp.bfloat16)

    pltpu.make_async_copy(p_hbm, pv, p_sem).wait()
    for l in range(L):
        for gu in range(2):
            rows = xs[pl.ds((gu * L + l) * HB, HB)].reshape(ROWS, W)
            proj = lax.dot_general(
                pv[l], rows, (((1,), (1,)), ((), ())), preferred_element_type=jnp.float32
            )
            for a in range(NX):
                for b in range(NY):
                    t = (a * NY + b) * TC
                    part[b, a, l, :, pl.ds(gu * HALFW, ROWS)] = proj[t:t + TC]

    pl.semaphore_wait(barrier, R - 1 + NY)

    def weights(i):
        to = (me + i) % R
        return pltpu.make_async_remote_copy(
            src_ref=msg.at[to], dst_ref=got.at[me], send_sem=w_send.at[i], recv_sem=w_recv.at[me],
            device_id={"row": to}, device_id_type=MESH,
        )

    def hiddens(i):
        to = (me + i) % R
        return pltpu.make_async_remote_copy(
            src_ref=hsend.at[to], dst_ref=hgot.at[me], send_sem=h_send.at[i], recv_sem=h_recv.at[me],
            device_id={"row": to}, device_id_type=MESH,
        )

    def start_weights(i, _):
        weights(i).start()
        return _

    def phase_a(dy):
        to = (y + dy) % NY
        return pltpu.make_async_remote_copy(
            src_ref=part.at[to], dst_ref=in_a.at[dy - 1], send_sem=a_send.at[dy - 1], recv_sem=a_recv.at[dy - 1],
            device_id={"col": xh * NY + to}, device_id_type=MESH,
        )

    for dy in range(1, NY):
        phase_a(dy).start()
    lax.fori_loop(1, R, start_weights, 0)

    def place(p, rows_of):
        for c in range(TILES):
            stage[c] = rows_of[p, :, pl.ds(c * LANES, LANES)].astype(jnp.float32)
        for c in range(TILES):
            for q in range(2 * L):
                lined[q, c, pl.ds(p * HB, HB), :] = stage[c, pl.ds(q * HB, HB), :]

    place(me, msg)

    for dy in range(1, NY):
        phase_a(dy).wait()
    summed[...] = part[y] + in_a[0] + in_a[1] + in_a[2]
    phase_b = pltpu.make_async_remote_copy(
        src_ref=summed.at[1 - xh], dst_ref=in_b, send_sem=b_send, recv_sem=b_recv,
        device_id={"col": partner}, device_id_type=MESH,
    )
    phase_b.start()
    phase_b.wait()
    total = summed[xh] + in_b[...]
    left, right = total[:, :, :HALFW], total[:, :, HALFW:]
    act = left / (1.0 + jnp.exp(-left)) * right
    stacked = jnp.concatenate(
        [act[l, :, g * LANES:(g + 1) * LANES] for g in range(4) for l in range(L)], axis=0
    )
    hidt[...] = stacked.T
    for k in range(C):
        hsend[k] = hidt[pl.ds(k, 4, stride=C), :].astype(jnp.bfloat16)

    def start_hidden(i, _):
        hiddens(i).start()
        return _

    lax.fori_loop(1, R, start_hidden, 0)
    hgot[me] = hsend[me]

    for i in range(1, R):
        hiddens(i).wait_send()
    for i in range(1, R):
        src = (me + i) % R
        pltpu.make_async_remote_copy(
            src_ref=hsend.at[0], dst_ref=hgot.at[src], send_sem=h_send.at[i], recv_sem=h_recv.at[src],
            device_id={"row": src}, device_id_type=MESH,
        ).wait_recv()
    for g in (3, 0, 1, 2):
        n = 2 if g == 3 else 4
        for p in range(R):
            piece = hgot[p].astype(jnp.float32)
            order[pl.ds(p * HB + 4 * g, n), :] = pltpu.roll(piece, (LANES - 32 * g) % LANES, 1)[:n]
    flat = order[...].T
    for l in range(L):
        hid[l] = flat[l * TC:(l + 1) * TC, :ROWS].astype(jnp.bfloat16)

    def arrived(i, _):
        src = (me + R - i) % R
        pltpu.make_async_remote_copy(
            src_ref=msg.at[0], dst_ref=got.at[src], send_sem=w_send.at[i], recv_sem=w_recv.at[src],
            device_id={"row": src}, device_id_type=MESH,
        ).wait_recv()
        place(src, got)
        return _

    lax.fori_loop(1, R, arrived, 0)
    for l in range(L):
        for c in range(TILES):
            gate[l, :, pl.ds(c * LANES, LANES)] = lined[l, c].astype(jnp.bfloat16)
            up[l, :, pl.ds(c * LANES, LANES)] = lined[L + l, c].astype(jnp.bfloat16)

    def sent(i, _):
        weights(i).wait_send()
        return _

    lax.fori_loop(1, R, sent, 0)


def emit(gate_in, up_in, hid_in, gate, up, hid, sems):
    copies = [
        pltpu.make_async_copy(a, b, sems.at[i])
        for i, (a, b) in enumerate(((gate_in, gate), (up_in, up), (hid_in, hid)))
    ]
    for copy in copies:
        copy.start()
    for copy in copies:
        copy.wait()


def body(joined, probes):
    x = jnp.transpose(joined, (0, 2, 3, 1, 4)).reshape(L, HB, 2, C, W)
    hbm = pl.BlockSpec(memory_space=pltpu.HBM)
    vmem = pl.BlockSpec(memory_space=pltpu.VMEM)
    dma = pltpu.SemaphoreType.DMA
    f32, bf16 = jnp.float32, jnp.bfloat16
    outs = (
        jax.ShapeDtypeStruct((L, ROWS, W), bf16),
        jax.ShapeDtypeStruct((L, ROWS, W), bf16),
        jax.ShapeDtypeStruct((L, TC, ROWS), bf16),
    )
    x = pltpu.with_memory_space_constraint(x, pltpu.HBM)
    probes = pltpu.with_memory_space_constraint(probes, pltpu.HBM)
    held = pl.pallas_call(
        exchange,
        out_shape=outs,
        in_specs=[hbm, hbm],
        out_specs=(vmem, vmem, vmem),
        scratch_shapes=[
            pltpu.VMEM((J, C, W), bf16),
            pltpu.VMEM((L, T, W), bf16),
            pltpu.VMEM((TILES, J * PITCH, LANES), f32),
            pltpu.VMEM((C, J, W), bf16),
            pltpu.VMEM((R, J, W), bf16),
            pltpu.VMEM((TILES, J, LANES), f32),
            pltpu.VMEM((2 * L, TILES, ROWS, LANES), f32),
            pltpu.VMEM((NY, NX, L, TC, 2 * HALFW), f32),
            pltpu.VMEM((NY - 1, NX, L, TC, 2 * HALFW), f32),
            pltpu.VMEM((NX, L, TC, 2 * HALFW), f32),
            pltpu.VMEM((L, TC, 2 * HALFW), f32),
            pltpu.VMEM((LANES, LANES), f32),
            pltpu.VMEM((C, 4, LANES), bf16),
            pltpu.VMEM((R, 4, LANES), bf16),
            pltpu.VMEM((512, LANES), f32),
            dma((2 * L,)), dma,
            dma((R,)), dma((R,)),
            dma((NY - 1,)), dma((NY - 1,)),
            dma, dma,
            dma((R,)), dma((R,)),
        ],
        compiler_params=pltpu.CompilerParams(
            collective_id=0, has_side_effects=True, vmem_limit_bytes=32 * 2**20
        ),
        name="exchange",
    )(x, probes)
    return pl.pallas_call(
        emit,
        out_shape=outs,
        in_specs=[vmem, vmem, vmem],
        out_specs=(hbm, hbm, hbm),
        scratch_shapes=[dma((3,))],
        compiler_params=pltpu.CompilerParams(vmem_limit_bytes=2 * 2**20),
        name="emit",
    )(*held)


def solution(mesh):
    return jax.shard_map(
        body,
        mesh=mesh,
        in_specs=(P(None, None, "row", None, "col"), P(None, None, "col")),
        out_specs=(P(None, "row", "col"), P(None, "row", "col"), P(None, "col", "row")),
        check_vma=False,
    )
```

```python
import functools

import jax
import jax.numpy as jnp
from jax import lax
from jax.experimental import pallas as pl
from jax.experimental.pallas import tpu as pltpu
from jax.sharding import PartitionSpec as P

MESH = pl.DeviceIdType.MESH
L, C, R, B, W = 2, 32, 32, 28, 512
HB = B // 2
J = L * B
T = 128
NY, NX, NZ = 4, 2, 8
TURN = 25
GROUP = 4
EARLY = 24
BEFORE = 6
TC = T // (NY * NX)
PITCH = C + 1
LANES = 128
TILES = W // LANES
HALFW = 512
ROWS = C * HB


def exchange(
    x_hbm, p_hbm, gate, up, hid, xs, pv, spread, msg, got, stage, lined, part, in_a, summed, in_b, hidt, hsend, hgot, order,
    load_sem, p_sem, w_send, w_recv, a_send, a_recv, b_send, b_recv, h_send, h_recv,
):
    me = lax.axis_index("row")
    col = lax.axis_index("col")
    xh, y = lax.div(col, NY), lax.rem(col, NY)
    xl, z, core = lax.div(me, 2 * NZ), lax.rem(lax.div(me, 2), NZ), lax.rem(me, 2)

    def moved(step, sign):
        turn = lax.rem(step * TURN, R)
        dx, dz, dc = lax.div(turn, 2 * NZ), lax.rem(lax.div(turn, 2), NZ), lax.rem(turn, 2)
        there = lax.rem(z + NZ + sign * dz, NZ)
        return lax.rem(xl + dx, 2) * (2 * NZ) + there * 2 + lax.rem(core + dc, 2)

    for q in range(2 * L):
        pltpu.make_async_copy(x_hbm.at[q % L, :, q // L], xs.at[pl.ds(q * HB, HB)], load_sem.at[q]).start()
    pltpu.make_async_copy(p_hbm, pv, p_sem).start()

    barrier = pltpu.get_barrier_semaphore()

    def hello(i, _):
        pl.semaphore_signal(barrier, inc=1, device_id={"row": lax.rem(me + i, R)}, device_id_type=MESH)
        return _

    lax.fori_loop(1, R, hello, 0)
    for dy in range(1, NY):
        pl.semaphore_signal(barrier, inc=1, device_id={"col": xh * NY + lax.rem(y + dy, NY)}, device_id_type=MESH)
    partner = (1 - xh) * NY + y
    pl.semaphore_signal(barrier, inc=1, device_id={"col": partner}, device_id_type=MESH)

    for q in range(2 * L):
        pltpu.make_async_copy(x_hbm.at[q % L, :, q // L], xs.at[pl.ds(q * HB, HB)], load_sem.at[q]).wait()
        for i in range(HB):
            j = q * HB + i
            rows = xs[j].astype(jnp.float32)
            for c in range(TILES):
                spread[c, pl.ds(j * PITCH, C), :] = rows[:, c * LANES:(c + 1) * LANES]
    for k in range(C):
        for c in range(TILES):
            msg[k, :, pl.ds(c * LANES, LANES)] = spread[c, pl.ds(k, J, stride=PITCH), :].astype(jnp.bfloat16)

    pl.semaphore_wait(barrier, R - 1 + NY)

    def start_weights(s, _):
        to = moved(s, 1)
        pltpu.make_async_remote_copy(
            src_ref=msg.at[to], dst_ref=got.at[me], send_sem=w_send, recv_sem=w_recv.at[lax.div(s - 1, GROUP)],
            device_id={"row": to}, device_id_type=MESH,
        ).start()
        return _

    def start_hidden(s, _):
        to = moved(s, 1)
        pltpu.make_async_remote_copy(
            src_ref=hsend.at[to], dst_ref=hgot.at[me], send_sem=h_send, recv_sem=h_recv,
            device_id={"row": to}, device_id_type=MESH,
        ).start()
        return _

    lax.fori_loop(1, EARLY + 1, start_weights, 0)

    pltpu.make_async_copy(p_hbm, pv, p_sem).wait()
    for l in range(L):
        for gu in range(2):
            rows = xs[pl.ds((gu * L + l) * HB, HB)].reshape(ROWS, W)
            proj = lax.dot_general(
                pv[l], rows, (((1,), (1,)), ((), ())), preferred_element_type=jnp.float32
            )
            for a in range(NX):
                for b in range(NY):
                    t = (a * NY + b) * TC
                    part[b, a, l, :, pl.ds(gu * HALFW, ROWS)] = proj[t:t + TC]

    for dy in range(1, NY):
        to = lax.rem(y + dy, NY)
        pltpu.make_async_remote_copy(
            src_ref=part.at[to], dst_ref=in_a.at[dy - 1], send_sem=a_send, recv_sem=a_recv,
            device_id={"col": xh * NY + to}, device_id_type=MESH,
        ).start()

    def place(p, rows_of):
        for c in range(TILES):
            stage[c] = rows_of[p, :, pl.ds(c * LANES, LANES)].astype(jnp.float32)
        for c in range(TILES):
            for q in range(2 * L):
                lined[q, c, pl.ds(p * HB, HB), :] = stage[c, pl.ds(q * HB, HB), :]

    place(me, msg)

    pltpu.make_async_copy(in_a, in_a, a_recv).wait()
    summed[...] = part[y] + in_a[0] + in_a[1] + in_a[2]
    phase_b = pltpu.make_async_remote_copy(
        src_ref=summed.at[1 - xh], dst_ref=in_b, send_sem=b_send, recv_sem=b_recv,
        device_id={"col": partner}, device_id_type=MESH,
    )
    phase_b.start()
    phase_b.wait_recv()
    total = summed[xh] + in_b[...]
    left, right = total[:, :, :HALFW], total[:, :, HALFW:]
    act = left / (1.0 + jnp.exp(-left)) * right
    stacked = jnp.concatenate(
        [act[l, :, g * LANES:(g + 1) * LANES] for g in range(4) for l in range(L)], axis=0
    )
    hidt[...] = stacked.T
    for k in range(C):
        hsend[k] = hidt[pl.ds(k, 4, stride=C), :].astype(jnp.bfloat16)

    lax.fori_loop(1, R, start_hidden, 0)
    lax.fori_loop(EARLY + 1, R, start_weights, 0)
    hgot[me] = hsend[me]

    def arrived(s, _):
        place(moved(s, -1), got)
        return _

    def group(g, _):
        pltpu.make_async_copy(got.at[pl.ds(0, GROUP)], got.at[pl.ds(0, GROUP)], w_recv.at[g]).wait()
        lax.fori_loop(g * GROUP + 1, g * GROUP + GROUP + 1, arrived, 0)
        return _

    whole = (R - 1) // GROUP
    lax.fori_loop(0, BEFORE, group, 0)
    pltpu.make_async_copy(hgot.at[pl.ds(0, R - 1)], hgot.at[pl.ds(0, R - 1)], h_recv).wait()
    for g in (3, 0, 1, 2):
        n = 2 if g == 3 else 4
        for p in range(R):
            piece = hgot[p].astype(jnp.float32)
            order[pl.ds(p * HB + 4 * g, n), :] = pltpu.roll(piece, (LANES - 32 * g) % LANES, 1)[:n]
    flat = order[...].T
    for l in range(L):
        hid[l] = flat[l * TC:(l + 1) * TC, :ROWS].astype(jnp.bfloat16)
    lax.fori_loop(BEFORE, whole, group, 0)
    rest = R - 1 - whole * GROUP
    pltpu.make_async_copy(got.at[pl.ds(0, rest)], got.at[pl.ds(0, rest)], w_recv.at[whole]).wait()
    lax.fori_loop(whole * GROUP + 1, R, arrived, 0)

    for l in range(L):
        for c in range(TILES):
            gate[l, :, pl.ds(c * LANES, LANES)] = lined[l, c].astype(jnp.bfloat16)
            up[l, :, pl.ds(c * LANES, LANES)] = lined[L + l, c].astype(jnp.bfloat16)

    pltpu.make_async_copy(msg.at[pl.ds(0, R - 1)], msg.at[pl.ds(0, R - 1)], w_send).wait()
    pltpu.make_async_copy(in_a, in_a, a_send).wait()
    phase_b.wait_send()
    pltpu.make_async_copy(hgot.at[pl.ds(0, R - 1)], hgot.at[pl.ds(0, R - 1)], h_send).wait()


def emit(gate_in, up_in, hid_in, gate, up, hid, sems):
    copies = [
        pltpu.make_async_copy(a, b, sems.at[i])
        for i, (a, b) in enumerate(((gate_in, gate), (up_in, up), (hid_in, hid)))
    ]
    for copy in copies:
        copy.start()
    for copy in copies:
        copy.wait()


def body(joined, probes):
    x = jnp.transpose(joined, (0, 2, 3, 1, 4)).reshape(L, HB, 2, C, W)
    hbm = pl.BlockSpec(memory_space=pltpu.HBM)
    vmem = pl.BlockSpec(memory_space=pltpu.VMEM)
    dma = pltpu.SemaphoreType.DMA
    f32, bf16 = jnp.float32, jnp.bfloat16
    outs = (
        jax.ShapeDtypeStruct((L, ROWS, W), bf16),
        jax.ShapeDtypeStruct((L, ROWS, W), bf16),
        jax.ShapeDtypeStruct((L, TC, ROWS), bf16),
    )
    x = pltpu.with_memory_space_constraint(x, pltpu.HBM)
    probes = pltpu.with_memory_space_constraint(probes, pltpu.HBM)
    held = pl.pallas_call(
        exchange,
        out_shape=outs,
        in_specs=[hbm, hbm],
        out_specs=(vmem, vmem, vmem),
        scratch_shapes=[
            pltpu.VMEM((J, C, W), bf16),
            pltpu.VMEM((L, T, W), bf16),
            pltpu.VMEM((TILES, J * PITCH, LANES), f32),
            pltpu.VMEM((C, J, W), bf16),
            pltpu.VMEM((R, J, W), bf16),
            pltpu.VMEM((TILES, J, LANES), f32),
            pltpu.VMEM((2 * L, TILES, ROWS, LANES), f32),
            pltpu.VMEM((NY, NX, L, TC, 2 * HALFW), f32),
            pltpu.VMEM((NY - 1, NX, L, TC, 2 * HALFW), f32),
            pltpu.VMEM((NX, L, TC, 2 * HALFW), f32),
            pltpu.VMEM((L, TC, 2 * HALFW), f32),
            pltpu.VMEM((LANES, LANES), f32),
            pltpu.VMEM((C, 4, LANES), bf16),
            pltpu.VMEM((R, 4, LANES), bf16),
            pltpu.VMEM((512, LANES), f32),
            dma((2 * L,)), dma,
            dma, dma((-(-(R - 1) // GROUP),)),
            dma, dma,
            dma, dma,
            dma, dma,
        ],
        compiler_params=pltpu.CompilerParams(
            collective_id=0, has_side_effects=True, vmem_limit_bytes=32 * 2**20
        ),
        name="exchange",
    )(x, probes)
    return pl.pallas_call(
        emit,
        out_shape=outs,
        in_specs=[vmem, vmem, vmem],
        out_specs=(hbm, hbm, hbm),
        scratch_shapes=[dma((3,))],
        compiler_params=pltpu.CompilerParams(vmem_limit_bytes=2 * 2**20),
        name="emit",
    )(*held)


def solution(mesh):
    return jax.shard_map(
        body,
        mesh=mesh,
        in_specs=(P(None, None, "row", None, "col"), P(None, None, "col")),
        out_specs=(P(None, "row", "col"), P(None, "row", "col"), P(None, "col", "row")),
        check_vma=False,
    )
```

```python
import functools

import jax
import jax.numpy as jnp
from jax import lax
from jax.experimental import pallas as pl
from jax.experimental.pallas import tpu as pltpu
from jax.sharding import PartitionSpec as P

MESH = pl.DeviceIdType.MESH
L, C, R, B, W = 2, 32, 32, 28, 512
HB = B // 2
J = L * B
T = 128
NY, NX, NZ = 4, 2, 8
FIRST = (2, 14, 19, 31, 3, 15, 18, 30)
ORDER = FIRST + tuple(n for n in (25 * s % 32 for s in range(1, 32)) if n not in FIRST)
NEAR = 11
SENDNEAR = len(FIRST)
GROUP = 4
EARLY = 22
BEFORE = 5
AHEAD = 2
LIMIT = 24
BONUS = (8, 0, 0, 0, 0, 0, 0, 0)
TC = T // (NY * NX)
PITCH = C + 1
LANES = 128
TILES = W // LANES
HALFW = 512
ROWS = C * HB


def plan(z, bonus):
    def rank(n):
        return n - (bonus[(z + ORDER[n] // 2) % NZ] if n >= LIMIT else 0)

    return [ORDER[n] + R * (n // GROUP) for n in sorted(range(R - 1), key=rank)]


def exchange(
    x_hbm, p_hbm, lined, hid, xs, pv, spread, msg, got, stage, part, in_a, summed, in_b, hidt, hsend, hgot, order,
    load_sem, p_sem, w_send, w_recv, a_send, a_recv, b_send, b_recv, h_send, h_recv, near_sem, far_sem,
):
    me = lax.axis_index("row")
    col = lax.axis_index("col")
    xh, y = lax.div(col, NY), lax.rem(col, NY)
    xl, z, core = lax.div(me, 2 * NZ), lax.rem(lax.div(me, 2), NZ), lax.rem(me, 2)

    def moved(turn, sign):
        dx, dz, dc = lax.div(turn, 2 * NZ), lax.rem(lax.div(turn, 2), NZ), lax.rem(turn, 2)
        there = lax.rem(z + NZ + sign * dz, NZ)
        return lax.rem(xl + dx, 2) * (2 * NZ) + there * 2 + lax.rem(core + dc, 2)

    for q in range(2 * L):
        pltpu.make_async_copy(x_hbm.at[q % L, :, q // L], xs.at[pl.ds(q * HB, HB)], load_sem.at[q]).start()
    pltpu.make_async_copy(p_hbm, pv, p_sem).start()

    barrier = pltpu.get_barrier_semaphore()

    partner = (1 - xh) * NY + y
    for n in (n for n in ORDER if (n // 2 + 1) % NZ <= 2):
        pl.semaphore_signal(barrier, inc=1, device_id={"row": moved(n, 1)}, device_id_type=MESH)
    pl.semaphore_signal(barrier, inc=1, device_id={"col": partner}, device_id_type=MESH)
    for dy in range(1, NY):
        pl.semaphore_signal(barrier, inc=1, device_id={"col": xh * NY + lax.rem(y + dy, NY)}, device_id_type=MESH)

    for q in range(2 * L):
        pltpu.make_async_copy(x_hbm.at[q % L, :, q // L], xs.at[pl.ds(q * HB, HB)], load_sem.at[q]).wait()
        for i in range(HB):
            j = q * HB + i
            rows = xs[j].astype(jnp.float32)
            for c in range(TILES):
                spread[c, pl.ds(j * PITCH, C), :] = rows[:, c * LANES:(c + 1) * LANES]
    def build(k):
        for c in range(TILES):
            msg[k, :, pl.ds(c * LANES, LANES)] = spread[c, pl.ds(k, J, stride=PITCH), :].astype(jnp.bfloat16)

    plans = [plan(n, BONUS) for n in range(NZ)]

    def choice(n):
        options = [p[n] for p in plans]
        code = jnp.int32(options[0])
        for at, option in enumerate(options):
            if option != options[0]:
                code = jnp.where(z == at, jnp.int32(option), code)
        return moved(lax.rem(code, R), 1), lax.div(code, R)

    chosen = [choice(n) for n in range(R - 1)]

    def start_weights(n):
        to, which = chosen[n]
        pltpu.make_async_remote_copy(
            src_ref=msg.at[to], dst_ref=got.at[me], send_sem=w_send, recv_sem=w_recv.at[which],
            device_id={"row": to}, device_id_type=MESH,
        ).start()

    def start_hidden(n):
        to, _ = chosen[n]
        pltpu.make_async_remote_copy(
            src_ref=hsend.at[to], dst_ref=hgot.at[me], send_sem=h_send, recv_sem=h_recv,
            device_id={"row": to}, device_id_type=MESH,
        ).start()

    def send(first, last):
        for n in range(first, last):
            if n + AHEAD < R - 1:
                build(chosen[n + AHEAD][0])
            start_weights(n)

    def tell(sem, steps):
        for turn in (2 * steps, 2 * (NZ - steps)):
            pl.semaphore_signal(sem, inc=1, device_id={"row": moved(turn, 1)}, device_id_type=MESH)

    for n in range(AHEAD):
        build(chosen[n][0])
    pl.semaphore_wait(barrier, NEAR + NY)
    tell(near_sem, 1)
    send(0, SENDNEAR)
    pl.semaphore_wait(near_sem, 2)
    tell(far_sem, 2)
    pltpu.make_async_copy(p_hbm, pv, p_sem).wait()
    for l in range(L):
        for gu in range(2):
            rows = xs[pl.ds((gu * L + l) * HB, HB)].reshape(ROWS, W)
            proj = lax.dot_general(
                pv[l], rows, (((1,), (1,)), ((), ())), preferred_element_type=jnp.float32
            )
            for a in range(NX):
                for b in range(NY):
                    t = (a * NY + b) * TC
                    part[l, b, a, :, pl.ds(gu * HALFW, ROWS)] = proj[t:t + TC]
        for dy in range(1, NY):
            to = lax.rem(y + dy, NY)
            pltpu.make_async_remote_copy(
                src_ref=part.at[l, to], dst_ref=in_a.at[l, dy - 1], send_sem=a_send, recv_sem=a_recv.at[l],
                device_id={"col": xh * NY + to}, device_id_type=MESH,
            ).start()
    for n in range(EARLY + AHEAD, R - 1):
        build(chosen[n][0])
    build(me)
    pl.semaphore_wait(far_sem, 2)
    send(SENDNEAR, EARLY)

    def place(p, rows_of):
        for c in range(TILES):
            stage[c] = rows_of[p, :, pl.ds(c * LANES, LANES)].astype(jnp.float32)
        for c in range(TILES):
            for q in range(2 * L):
                lined[q, c, pl.ds(p * HB, HB), :] = stage[c, pl.ds(q * HB, HB), :]

    place(me, msg)

    phase_b = []
    for l in range(L):
        pltpu.make_async_copy(in_a.at[l], in_a.at[l], a_recv.at[l]).wait()
        summed[l] = part[l, y] + in_a[l, 0] + in_a[l, 1] + in_a[l, 2]
        phase_b.append(pltpu.make_async_remote_copy(
            src_ref=summed.at[l, 1 - xh], dst_ref=in_b.at[l], send_sem=b_send.at[l], recv_sem=b_recv.at[l],
            device_id={"col": partner}, device_id_type=MESH,
        ))
        phase_b[l].start()
    act = []
    for l in range(L):
        phase_b[l].wait_recv()
        total = summed[l, xh] + in_b[l]
        left, right = total[:, :HALFW], total[:, HALFW:]
        act.append(left / (1.0 + jnp.exp(-left)) * right)
    stacked = jnp.concatenate(
        [act[l][:, g * LANES:(g + 1) * LANES] for g in range(4) for l in range(L)], axis=0
    )
    hidt[...] = stacked.T
    for k in range(C):
        hsend[k] = hidt[pl.ds(k, 4, stride=C), :].astype(jnp.bfloat16)

    for n in range(R - 1):
        start_hidden(n)
    for n in range(EARLY, R - 1):
        start_weights(n)
    hgot[me] = hsend[me]

    def groups(first, last):
        for g in range(first, last):
            turns = ORDER[g * GROUP:(g + 1) * GROUP]
            many = pl.ds(0, len(turns))
            pltpu.make_async_copy(got.at[many], got.at[many], w_recv.at[g]).wait()

            def arrived(i, _):
                turn = jnp.int32(turns[0])
                for n, other in enumerate(turns[1:]):
                    turn = jnp.where(i > n, jnp.int32(other), turn)
                place(moved(turn, -1), got)
                return _

            lax.fori_loop(0, len(turns), arrived, 0)

    groups(0, BEFORE)
    pltpu.make_async_copy(hgot.at[pl.ds(0, R - 1)], hgot.at[pl.ds(0, R - 1)], h_recv).wait()
    for g in (3, 0, 1, 2):
        n = 2 if g == 3 else 4
        for p in range(R):
            piece = hgot[p].astype(jnp.float32)
            order[pl.ds(p * HB + 4 * g, n), :] = pltpu.roll(piece, (LANES - 32 * g) % LANES, 1)[:n]
    flat = order[...].T
    for l in range(L):
        hid[l] = flat[l * TC:(l + 1) * TC, :ROWS].astype(jnp.bfloat16)
    groups(BEFORE, -(-(R - 1) // GROUP))

    pltpu.make_async_copy(msg.at[pl.ds(0, R - 1)], msg.at[pl.ds(0, R - 1)], w_send).wait()
    pltpu.make_async_copy(in_a, in_a, a_send).wait()
    for copy in phase_b:
        copy.wait_send()
    pltpu.make_async_copy(hgot.at[pl.ds(0, R - 1)], hgot.at[pl.ds(0, R - 1)], h_send).wait()


def emit(lined, hid_in, gate, up, hid, rows, sems):
    copies = [pltpu.make_async_copy(hid_in, hid, sems.at[2 * L])]
    copies[0].start()
    for q in range(2 * L):
        for c in range(TILES):
            rows[q, :, pl.ds(c * LANES, LANES)] = lined[q, c].astype(jnp.bfloat16)
        copies.append(pltpu.make_async_copy(rows.at[q], (gate, up)[q // L].at[q % L], sems.at[q]))
        copies[-1].start()
    for copy in copies:
        copy.wait()


def body(joined, probes):
    x = jnp.transpose(joined, (0, 2, 3, 1, 4)).reshape(L, HB, 2, C, W)
    hbm = pl.BlockSpec(memory_space=pltpu.HBM)
    vmem = pl.BlockSpec(memory_space=pltpu.VMEM)
    dma = pltpu.SemaphoreType.DMA
    f32, bf16 = jnp.float32, jnp.bfloat16
    outs = (
        jax.ShapeDtypeStruct((L, ROWS, W), bf16),
        jax.ShapeDtypeStruct((L, ROWS, W), bf16),
        jax.ShapeDtypeStruct((L, TC, ROWS), bf16),
    )
    x = pltpu.with_memory_space_constraint(x, pltpu.HBM)
    probes = pltpu.with_memory_space_constraint(probes, pltpu.HBM)
    held = pl.pallas_call(
        exchange,
        out_shape=(jax.ShapeDtypeStruct((2 * L, TILES, ROWS, LANES), f32), outs[2]),
        in_specs=[hbm, hbm],
        out_specs=(vmem, vmem),
        scratch_shapes=[
            pltpu.VMEM((J, C, W), bf16),
            pltpu.VMEM((L, T, W), bf16),
            pltpu.VMEM((TILES, J * PITCH, LANES), f32),
            pltpu.VMEM((C, J, W), bf16),
            pltpu.VMEM((R, J, W), bf16),
            pltpu.VMEM((TILES, J, LANES), f32),
            pltpu.VMEM((L, NY, NX, TC, 2 * HALFW), f32),
            pltpu.VMEM((L, NY - 1, NX, TC, 2 * HALFW), f32),
            pltpu.VMEM((L, NX, TC, 2 * HALFW), f32),
            pltpu.VMEM((L, TC, 2 * HALFW), f32),
            pltpu.VMEM((LANES, LANES), f32),
            pltpu.VMEM((C, 4, LANES), bf16),
            pltpu.VMEM((R, 4, LANES), bf16),
            pltpu.VMEM((512, LANES), f32),
            dma((2 * L,)), dma,
            dma, dma((-(-(R - 1) // GROUP),)),
            dma, dma((L,)),
            dma((L,)), dma((L,)),
            dma, dma,
            pltpu.SemaphoreType.REGULAR, pltpu.SemaphoreType.REGULAR,
        ],
        compiler_params=pltpu.CompilerParams(
            collective_id=0, has_side_effects=True, vmem_limit_bytes=32 * 2**20
        ),
        name="exchange",
    )(x, probes)
    return pl.pallas_call(
        emit,
        out_shape=outs,
        in_specs=[vmem, vmem],
        out_specs=(hbm, hbm, hbm),
        scratch_shapes=[pltpu.VMEM((2 * L, ROWS, W), bf16), dma((2 * L + 1,))],
        compiler_params=pltpu.CompilerParams(vmem_limit_bytes=4 * 2**20),
        name="emit",
    )(*held)


def solution(mesh):
    return jax.shard_map(
        body,
        mesh=mesh,
        in_specs=(P(None, None, "row", None, "col"), P(None, None, "col")),
        out_specs=(P(None, "row", "col"), P(None, "row", "col"), P(None, "col", "row")),
        check_vma=False,
    )
```

```python
import functools

import jax
import jax.numpy as jnp
from jax import lax
from jax.experimental import pallas as pl
from jax.experimental.pallas import tpu as pltpu
from jax.sharding import PartitionSpec as P

MESH = pl.DeviceIdType.MESH
L, C, R, B, W = 2, 32, 32, 28, 512
HB = B // 2
J = L * B
T = 128
NY, NX, NZ = 4, 2, 8
FIRST = (2, 14, 19, 31)
NEXT = (4, 12, 21, 29)
ORDER = FIRST + NEXT + tuple(n for n in (25 * s % 32 for s in range(1, 32)) if n not in FIRST + NEXT)
NEAR = 11
SENDNEAR = len(FIRST)
SENDNEXT = SENDNEAR + len(NEXT)
GROUP = 4
EARLY = 22
MIDWAY = 5
BEFORE = 6
HIDDEN = (4, 3, 5, 2, 6, 1, 7)
AHEAD = 2
LIMIT = 24
BONUS = (8, 0, 0, 0, 0, 0, 0, 0)
TC = T // (NY * NX)
PITCH = C + 1
LANES = 128
TILES = W // LANES
HALFW = 512
ROWS = C * HB


def plan(z, bonus):
    def rank(n):
        return n - (bonus[(z + ORDER[n] // 2) % NZ] if n >= LIMIT else 0)

    return [ORDER[n] + R * (n // GROUP) for n in sorted(range(R - 1), key=rank)]


def exchange(
    x_hbm, p_hbm, lined, hid, xs, pv, spread, msg, got, stage, part, in_a, summed, in_b, hidt, hsend, hmid, hgot, order,
    load_sem, p_sem, w_send, w_recv, a_send, a_recv, b_send, b_recv, h_send, h_recv, m_send, m_recv, near_sem, far_sem,
):
    me = lax.axis_index("row")
    col = lax.axis_index("col")
    xh, y = lax.div(col, NY), lax.rem(col, NY)
    xl, z, core = lax.div(me, 2 * NZ), lax.rem(lax.div(me, 2), NZ), lax.rem(me, 2)

    def moved(turn, sign):
        dx, dz, dc = lax.div(turn, 2 * NZ), lax.rem(lax.div(turn, 2), NZ), lax.rem(turn, 2)
        there = lax.rem(z + NZ + sign * dz, NZ)
        return lax.rem(xl + dx, 2) * (2 * NZ) + there * 2 + lax.rem(core + dc, 2)

    for q in range(2 * L):
        pltpu.make_async_copy(x_hbm.at[q % L, :, q // L], xs.at[pl.ds(q * HB, HB)], load_sem.at[q]).start()
    pltpu.make_async_copy(p_hbm, pv, p_sem).start()

    barrier = pltpu.get_barrier_semaphore()

    partner = (1 - xh) * NY + y
    for n in (n for n in ORDER if (n // 2 + 1) % NZ <= 2):
        pl.semaphore_signal(barrier, inc=1, device_id={"row": moved(n, 1)}, device_id_type=MESH)
    pl.semaphore_signal(barrier, inc=1, device_id={"col": partner}, device_id_type=MESH)
    for dy in range(1, NY):
        pl.semaphore_signal(barrier, inc=1, device_id={"col": xh * NY + lax.rem(y + dy, NY)}, device_id_type=MESH)

    for q in range(2 * L):
        pltpu.make_async_copy(x_hbm.at[q % L, :, q // L], xs.at[pl.ds(q * HB, HB)], load_sem.at[q]).wait()
        for i in range(HB):
            j = q * HB + i
            rows = xs[j].astype(jnp.float32)
            for c in range(TILES):
                spread[c, pl.ds(j * PITCH, C), :] = rows[:, c * LANES:(c + 1) * LANES]
    def build(k):
        for c in range(TILES):
            msg[k, :, pl.ds(c * LANES, LANES)] = spread[c, pl.ds(k, J, stride=PITCH), :].astype(jnp.bfloat16)

    plans = [plan(n, BONUS) for n in range(NZ)]

    def choice(n):
        options = [p[n] for p in plans]
        code = jnp.int32(options[0])
        for at, option in enumerate(options):
            if option != options[0]:
                code = jnp.where(z == at, jnp.int32(option), code)
        return moved(lax.rem(code, R), 1), lax.div(code, R)

    chosen = [choice(n) for n in range(R - 1)]

    def start_weights(n):
        to, which = chosen[n]
        pltpu.make_async_remote_copy(
            src_ref=msg.at[to], dst_ref=got.at[me], send_sem=w_send, recv_sem=w_recv.at[which],
            device_id={"row": to}, device_id_type=MESH,
        ).start()

    seat = xl * 2 + core

    def start_hidden(dz):
        there = lax.rem(z + dz, NZ)
        pltpu.make_async_remote_copy(
            src_ref=hsend.at[there], dst_ref=hmid.at[z], send_sem=h_send, recv_sem=h_recv,
            device_id={"row": moved(2 * dz, 1)}, device_id_type=MESH,
        ).start()

    def pass_hidden(turn):
        to = moved(turn, 1)
        other = lax.div(to, 2 * NZ) * 2 + lax.rem(to, 2)
        pltpu.make_async_remote_copy(
            src_ref=hmid.at[:, other], dst_ref=hgot.at[seat], send_sem=m_send, recv_sem=m_recv,
            device_id={"row": to}, device_id_type=MESH,
        ).start()

    def send(first, last):
        for n in range(first, last):
            if n + AHEAD < R - 1:
                build(chosen[n + AHEAD][0])
            start_weights(n)

    def tell(sem, steps):
        for turn in (2 * steps, 2 * (NZ - steps)):
            pl.semaphore_signal(sem, inc=1, device_id={"row": moved(turn, 1)}, device_id_type=MESH)

    for n in range(AHEAD):
        build(chosen[n][0])
    pl.semaphore_wait(barrier, NEAR + NY)
    tell(near_sem, 1)
    send(0, SENDNEAR)
    pl.semaphore_wait(near_sem, 2)
    tell(far_sem, 2)
    send(SENDNEAR, SENDNEXT)
    pltpu.make_async_copy(p_hbm, pv, p_sem).wait()
    for l in range(L):
        for gu in range(2):
            rows = xs[pl.ds((gu * L + l) * HB, HB)].reshape(ROWS, W)
            proj = lax.dot_general(
                pv[l], rows, (((1,), (1,)), ((), ())), preferred_element_type=jnp.float32
            )
            for a in range(NX):
                for b in range(NY):
                    t = (a * NY + b) * TC
                    part[l, b, a, :, pl.ds(gu * HALFW, ROWS)] = proj[t:t + TC]
        for dy in range(1, NY):
            to = lax.rem(y + dy, NY)
            pltpu.make_async_remote_copy(
                src_ref=part.at[l, to], dst_ref=in_a.at[l, dy - 1], send_sem=a_send, recv_sem=a_recv.at[l],
                device_id={"col": xh * NY + to}, device_id_type=MESH,
            ).start()
    for n in range(EARLY + AHEAD, R - 1):
        build(chosen[n][0])
    build(me)
    pl.semaphore_wait(far_sem, 2)
    send(SENDNEXT, EARLY)

    def place(p, rows_of):
        for c in range(TILES):
            stage[c] = rows_of[p, :, pl.ds(c * LANES, LANES)].astype(jnp.float32)
        for c in range(TILES):
            for q in range(2 * L):
                lined[q, c, pl.ds(p * HB, HB), :] = stage[c, pl.ds(q * HB, HB), :]

    place(me, msg)

    phase_b = []
    for l in range(L):
        pltpu.make_async_copy(in_a.at[l], in_a.at[l], a_recv.at[l]).wait()
        summed[l] = part[l, y] + in_a[l, 0] + in_a[l, 1] + in_a[l, 2]
        phase_b.append(pltpu.make_async_remote_copy(
            src_ref=summed.at[l, 1 - xh], dst_ref=in_b.at[l], send_sem=b_send.at[l], recv_sem=b_recv.at[l],
            device_id={"col": partner}, device_id_type=MESH,
        ))
        phase_b[l].start()
    act = []
    for l in range(L):
        phase_b[l].wait_recv()
        total = summed[l, xh] + in_b[l]
        left, right = total[:, :HALFW], total[:, HALFW:]
        act.append(left / (1.0 + jnp.exp(-left)) * right)
    stacked = jnp.concatenate(
        [act[l][:, g * LANES:(g + 1) * LANES] for g in range(4) for l in range(L)], axis=0
    )
    hidt[...] = stacked.T
    for k in range(C):
        hsend[k // 2 % NZ, k // (2 * NZ) * 2 + k % 2] = hidt[pl.ds(k, 4, stride=C), :].astype(jnp.bfloat16)

    for dz in HIDDEN:
        start_hidden(dz)
    for n in range(EARLY, R - 1):
        start_weights(n)
    hmid[z] = hsend[z]

    def groups(first, last):
        for g in range(first, last):
            turns = ORDER[g * GROUP:(g + 1) * GROUP]
            many = pl.ds(0, len(turns))
            pltpu.make_async_copy(got.at[many], got.at[many], w_recv.at[g]).wait()

            def arrived(i, _):
                turn = jnp.int32(turns[0])
                for n, other in enumerate(turns[1:]):
                    turn = jnp.where(i > n, jnp.int32(other), turn)
                place(moved(turn, -1), got)
                return _

            lax.fori_loop(0, len(turns), arrived, 0)

    groups(0, MIDWAY)
    pltpu.make_async_copy(hmid.at[pl.ds(0, NZ - 1)], hmid.at[pl.ds(0, NZ - 1)], h_recv).wait()
    for turn in (1, 2 * NZ, 2 * NZ + 1):
        pass_hidden(turn)
    hgot[seat] = hmid[:, seat]
    groups(MIDWAY, BEFORE)
    pltpu.make_async_copy(hgot.at[pl.ds(0, 3)], hgot.at[pl.ds(0, 3)], m_recv).wait()
    for g in (3, 0, 1, 2):
        n = 2 if g == 3 else 4
        for p in range(R):
            piece = hgot[p // (2 * NZ) * 2 + p % 2, p // 2 % NZ].astype(jnp.float32)
            order[pl.ds(p * HB + 4 * g, n), :] = pltpu.roll(piece, (LANES - 32 * g) % LANES, 1)[:n]
    flat = order[...].T
    for l in range(L):
        hid[l] = flat[l * TC:(l + 1) * TC, :ROWS].astype(jnp.bfloat16)
    groups(BEFORE, -(-(R - 1) // GROUP))

    pltpu.make_async_copy(msg.at[pl.ds(0, R - 1)], msg.at[pl.ds(0, R - 1)], w_send).wait()
    pltpu.make_async_copy(in_a, in_a, a_send).wait()
    for copy in phase_b:
        copy.wait_send()
    pltpu.make_async_copy(hmid.at[pl.ds(0, NZ - 1)], hmid.at[pl.ds(0, NZ - 1)], h_send).wait()
    pltpu.make_async_copy(hgot.at[pl.ds(0, 3)], hgot.at[pl.ds(0, 3)], m_send).wait()


def emit(lined, hid_in, gate, up, hid, rows, sems):
    copies = [pltpu.make_async_copy(hid_in, hid, sems.at[2 * L])]
    copies[0].start()
    for q in range(2 * L):
        for c in range(TILES):
            rows[q, :, pl.ds(c * LANES, LANES)] = lined[q, c].astype(jnp.bfloat16)
        copies.append(pltpu.make_async_copy(rows.at[q], (gate, up)[q // L].at[q % L], sems.at[q]))
        copies[-1].start()
    for copy in copies:
        copy.wait()


def body(joined, probes):
    x = jnp.transpose(joined, (0, 2, 3, 1, 4)).reshape(L, HB, 2, C, W)
    hbm = pl.BlockSpec(memory_space=pltpu.HBM)
    vmem = pl.BlockSpec(memory_space=pltpu.VMEM)
    dma = pltpu.SemaphoreType.DMA
    f32, bf16 = jnp.float32, jnp.bfloat16
    outs = (
        jax.ShapeDtypeStruct((L, ROWS, W), bf16),
        jax.ShapeDtypeStruct((L, ROWS, W), bf16),
        jax.ShapeDtypeStruct((L, TC, ROWS), bf16),
    )
    x = pltpu.with_memory_space_constraint(x, pltpu.HBM)
    probes = pltpu.with_memory_space_constraint(probes, pltpu.HBM)
    held = pl.pallas_call(
        exchange,
        out_shape=(jax.ShapeDtypeStruct((2 * L, TILES, ROWS, LANES), f32), outs[2]),
        in_specs=[hbm, hbm],
        out_specs=(vmem, vmem),
        scratch_shapes=[
            pltpu.VMEM((J, C, W), bf16),
            pltpu.VMEM((L, T, W), bf16),
            pltpu.VMEM((TILES, J * PITCH, LANES), f32),
            pltpu.VMEM((C, J, W), bf16),
            pltpu.VMEM((R, J, W), bf16),
            pltpu.VMEM((TILES, J, LANES), f32),
            pltpu.VMEM((L, NY, NX, TC, 2 * HALFW), f32),
            pltpu.VMEM((L, NY - 1, NX, TC, 2 * HALFW), f32),
            pltpu.VMEM((L, NX, TC, 2 * HALFW), f32),
            pltpu.VMEM((L, TC, 2 * HALFW), f32),
            pltpu.VMEM((LANES, LANES), f32),
            pltpu.VMEM((NZ, 4, 4, LANES), bf16),
            pltpu.VMEM((NZ, 4, 4, LANES), bf16),
            pltpu.VMEM((4, NZ, 4, LANES), bf16),
            pltpu.VMEM((512, LANES), f32),
            dma((2 * L,)), dma,
            dma, dma((-(-(R - 1) // GROUP),)),
            dma, dma((L,)),
            dma((L,)), dma((L,)),
            dma, dma,
            dma, dma,
            pltpu.SemaphoreType.REGULAR, pltpu.SemaphoreType.REGULAR,
        ],
        compiler_params=pltpu.CompilerParams(
            collective_id=0, has_side_effects=True, vmem_limit_bytes=32 * 2**20
        ),
        name="exchange",
    )(x, probes)
    return pl.pallas_call(
        emit,
        out_shape=outs,
        in_specs=[vmem, vmem],
        out_specs=(hbm, hbm, hbm),
        scratch_shapes=[pltpu.VMEM((2 * L, ROWS, W), bf16), dma((2 * L + 1,))],
        compiler_params=pltpu.CompilerParams(vmem_limit_bytes=4 * 2**20),
        name="emit",
    )(*held)


def solution(mesh):
    return jax.shard_map(
        body,
        mesh=mesh,
        in_specs=(P(None, None, "row", None, "col"), P(None, None, "col")),
        out_specs=(P(None, "row", "col"), P(None, "row", "col"), P(None, "col", "row")),
        check_vma=False,
    )
```

```python
import functools

import jax
import jax.numpy as jnp
from jax import lax
from jax.experimental import pallas as pl
from jax.experimental.pallas import tpu as pltpu
from jax.sharding import PartitionSpec as P

MESH = pl.DeviceIdType.MESH
L, C, R, B, W = 2, 32, 32, 28, 512
HB = B // 2
J = L * B
T = 128
NY, NX, NZ = 4, 2, 8
FIRST = (2, 14, 19, 31)
NEXT = (4, 12, 21, 29)
ORDER = FIRST + NEXT + tuple(n for n in (25 * s % 32 for s in range(1, 32)) if n not in FIRST + NEXT)
NEAR = 11
SENDNEAR = len(FIRST)
SENDNEXT = SENDNEAR + len(NEXT)
GROUP = 4
EARLY = 22
MIDWAY = 5
BEFORE = 6
HIDDEN = (4, 3, 5, 2, 6, 1, 7)
AHEAD = 2
CUTS = 2
LIMIT = 24
BONUS = (4, 0, 0, 0, 0, 0, 0, 0)
TC = T // (NY * NX)
PITCH = C + 1
LANES = 128
TILES = W // LANES
HALFW = 512
ROWS = C * HB


def plan(z, bonus):
    def rank(n):
        return n - (bonus[(z + ORDER[n] // 2) % NZ] if n >= LIMIT else 0)

    return [ORDER[n] + R * (n // GROUP) for n in sorted(range(R - 1), key=rank)]


def exchange(
    x_hbm, p_hbm, lined, hid, xs, pv, spread, msg, got, stage, part, in_a, summed, in_b, hidt, hsend, hmid, hgot, order,
    load_sem, p_sem, w_send, w_recv, a_send, a_recv, b_send, b_recv, h_send, h_recv, m_send, m_recv, near_sem, far_sem,
):
    me = lax.axis_index("row")
    col = lax.axis_index("col")
    xh, y = lax.div(col, NY), lax.rem(col, NY)
    xl, z, core = lax.div(me, 2 * NZ), lax.rem(lax.div(me, 2), NZ), lax.rem(me, 2)

    def moved(turn, sign):
        dx, dz, dc = lax.div(turn, 2 * NZ), lax.rem(lax.div(turn, 2), NZ), lax.rem(turn, 2)
        there = lax.rem(z + NZ + sign * dz, NZ)
        return lax.rem(xl + dx, 2) * (2 * NZ) + there * 2 + lax.rem(core + dc, 2)

    for q in range(2 * L):
        pltpu.make_async_copy(x_hbm.at[q % L, :, q // L], xs.at[pl.ds(q * HB, HB)], load_sem.at[q]).start()
    pltpu.make_async_copy(p_hbm, pv, p_sem).start()

    barrier = pltpu.get_barrier_semaphore()

    partner = (1 - xh) * NY + y
    for n in (n for n in ORDER if (n // 2 + 1) % NZ <= 2):
        pl.semaphore_signal(barrier, inc=1, device_id={"row": moved(n, 1)}, device_id_type=MESH)
    pl.semaphore_signal(barrier, inc=1, device_id={"col": partner}, device_id_type=MESH)
    for dy in range(1, NY):
        pl.semaphore_signal(barrier, inc=1, device_id={"col": xh * NY + lax.rem(y + dy, NY)}, device_id_type=MESH)

    for q in range(2 * L):
        pltpu.make_async_copy(x_hbm.at[q % L, :, q // L], xs.at[pl.ds(q * HB, HB)], load_sem.at[q]).wait()
        for i in range(HB):
            j = q * HB + i
            rows = xs[j].astype(jnp.float32)
            for c in range(TILES):
                spread[c, pl.ds(j * PITCH, C), :] = rows[:, c * LANES:(c + 1) * LANES]
    def build(k):
        for c in range(TILES):
            msg[k, :, pl.ds(c * LANES, LANES)] = spread[c, pl.ds(k, J, stride=PITCH), :].astype(jnp.bfloat16)

    plans = [plan(n, BONUS) for n in range(NZ)]

    def choice(n):
        options = [p[n] for p in plans]
        code = jnp.int32(options[0])
        for at, option in enumerate(options):
            if option != options[0]:
                code = jnp.where(z == at, jnp.int32(option), code)
        return moved(lax.rem(code, R), 1), lax.div(code, R)

    chosen = [choice(n) for n in range(R - 1)]

    def start_weights(n):
        to, which = chosen[n]
        pltpu.make_async_remote_copy(
            src_ref=msg.at[to], dst_ref=got.at[me], send_sem=w_send, recv_sem=w_recv.at[which],
            device_id={"row": to}, device_id_type=MESH,
        ).start()

    seat = xl * 2 + core

    def start_hidden(dz):
        there = lax.rem(z + dz, NZ)
        pltpu.make_async_remote_copy(
            src_ref=hsend.at[there], dst_ref=hmid.at[z], send_sem=h_send, recv_sem=h_recv,
            device_id={"row": moved(2 * dz, 1)}, device_id_type=MESH,
        ).start()

    def pass_hidden(turn):
        to = moved(turn, 1)
        other = lax.div(to, 2 * NZ) * 2 + lax.rem(to, 2)
        pltpu.make_async_remote_copy(
            src_ref=hmid.at[:, other], dst_ref=hgot.at[seat], send_sem=m_send, recv_sem=m_recv,
            device_id={"row": to}, device_id_type=MESH,
        ).start()

    def send(first, last):
        for n in range(first, last):
            if n + AHEAD < R - 1:
                build(chosen[n + AHEAD][0])
            start_weights(n)

    def tell(sem, steps):
        for turn in (2 * steps, 2 * (NZ - steps)):
            pl.semaphore_signal(sem, inc=1, device_id={"row": moved(turn, 1)}, device_id_type=MESH)

    for n in range(AHEAD):
        build(chosen[n][0])
    pl.semaphore_wait(barrier, NEAR + NY)
    tell(near_sem, 1)
    send(0, SENDNEAR)
    pl.semaphore_wait(near_sem, 2)
    tell(far_sem, 2)
    send(SENDNEAR, SENDNEXT)
    pltpu.make_async_copy(p_hbm, pv, p_sem).wait()
    for l in range(L):
        for gu in range(2):
            rows = xs[pl.ds((gu * L + l) * HB, HB)].reshape(ROWS, W)
            proj = lax.dot_general(
                pv[l], rows, (((1,), (1,)), ((), ())), preferred_element_type=jnp.float32
            )
            for a in range(NX):
                for b in range(NY):
                    t = (a * NY + b) * TC
                    part[l, b, a, :, pl.ds(gu * HALFW, ROWS)] = proj[t:t + TC]
        for dy in range(1, NY):
            to = lax.rem(y + dy, NY)
            pltpu.make_async_remote_copy(
                src_ref=part.at[l, to], dst_ref=in_a.at[l, dy - 1], send_sem=a_send, recv_sem=a_recv.at[l],
                device_id={"col": xh * NY + to}, device_id_type=MESH,
            ).start()
    for n in range(EARLY + AHEAD, R - 1):
        build(chosen[n][0])
    build(me)
    pl.semaphore_wait(far_sem, 2)
    send(SENDNEXT, EARLY)

    def place(p, rows_of):
        for c in range(TILES):
            stage[c, pl.ds(0, J), :] = rows_of[p, :, pl.ds(c * LANES, LANES)].astype(jnp.float32)
        for c in range(TILES):
            for q in range(2 * L):
                lined[q, c, pl.ds(p * HB, HB), :] = stage[c, pl.ds(q * HB, HB), :]

    place(me, msg)

    phase_b = []
    for l in range(L):
        pltpu.make_async_copy(in_a.at[l], in_a.at[l], a_recv.at[l]).wait()
        summed[l] = part[l, y] + in_a[l, 0] + in_a[l, 1] + in_a[l, 2]
        phase_b.append(pltpu.make_async_remote_copy(
            src_ref=summed.at[l, 1 - xh], dst_ref=in_b.at[l], send_sem=b_send.at[l], recv_sem=b_recv.at[l],
            device_id={"col": partner}, device_id_type=MESH,
        ))
        phase_b[l].start()
    act = []
    for l in range(L):
        phase_b[l].wait_recv()
        total = summed[l, xh] + in_b[l]
        left, right = total[:, :HALFW], total[:, HALFW:]
        act.append(left / (1.0 + jnp.exp(-left)) * right)
    stacked = jnp.concatenate(
        [act[l][:, g * LANES:(g + 1) * LANES] for g in range(4) for l in range(L)], axis=0
    )
    hidt[pl.ds(0, LANES), :] = stacked.T
    for k in range(C):
        hsend[k // 2 % NZ, k // (2 * NZ) * 2 + k % 2] = hidt[pl.ds(k, 4, stride=C), :].astype(jnp.bfloat16)

    for dz in HIDDEN:
        start_hidden(dz)
    for n in range(EARLY, R - 1):
        start_weights(n)
    hmid[z] = hsend[z]

    def groups(first, last):
        for g in range(first, last):
            turns = ORDER[g * GROUP:(g + 1) * GROUP]
            many = pl.ds(0, len(turns))
            pltpu.make_async_copy(got.at[many], got.at[many], w_recv.at[g]).wait()

            def arrived(i, _):
                turn = jnp.int32(turns[0])
                for n, other in enumerate(turns[1:]):
                    turn = jnp.where(i > n, jnp.int32(other), turn)
                place(moved(turn, -1), got)
                return _

            lax.fori_loop(0, len(turns), arrived, 0)

    groups(0, MIDWAY)
    pltpu.make_async_copy(hmid.at[pl.ds(0, NZ - 1)], hmid.at[pl.ds(0, NZ - 1)], h_recv).wait()
    for turn in (1, 2 * NZ, 2 * NZ + 1):
        pass_hidden(turn)
    hgot[seat] = hmid[:, seat]
    groups(MIDWAY, BEFORE)
    pltpu.make_async_copy(hgot.at[pl.ds(0, 3)], hgot.at[pl.ds(0, 3)], m_recv).wait()
    for g in (3, 0, 1, 2):
        n = 2 if g == 3 else 4
        for p in range(R):
            piece = hgot[p // (2 * NZ) * 2 + p % 2, p // 2 % NZ].astype(jnp.float32)
            order[pl.ds(p * HB + 4 * g, n), :] = pltpu.roll(piece, (LANES - 32 * g) % LANES, 1)[:n]
    flat = order[...].T
    for l in range(L):
        hid[l] = flat[l * TC:(l + 1) * TC, :ROWS].astype(jnp.bfloat16)
    groups(BEFORE, -(-(R - 1) // GROUP))

    pltpu.make_async_copy(msg.at[pl.ds(0, R - 1)], msg.at[pl.ds(0, R - 1)], w_send).wait()
    pltpu.make_async_copy(in_a, in_a, a_send).wait()
    for copy in phase_b:
        copy.wait_send()
    pltpu.make_async_copy(hmid.at[pl.ds(0, NZ - 1)], hmid.at[pl.ds(0, NZ - 1)], h_send).wait()
    pltpu.make_async_copy(hgot.at[pl.ds(0, 3)], hgot.at[pl.ds(0, 3)], m_send).wait()


def emit(lined, hid_in, gate, up, hid, rows, sems):
    copies = [pltpu.make_async_copy(hid_in, hid, sems.at[2 * L * CUTS])]
    copies[0].start()
    for q in range(2 * L):
        for n in range(CUTS):
            span = pl.ds(n * (ROWS // CUTS), ROWS // CUTS)
            for c in range(TILES):
                rows[q, span, pl.ds(c * LANES, LANES)] = lined[q, c, span].astype(jnp.bfloat16)
            copies.append(pltpu.make_async_copy(
                rows.at[q, span], (gate, up)[q // L].at[q % L, span], sems.at[q * CUTS + n]
            ))
            copies[-1].start()
    for copy in copies:
        copy.wait()


def body(joined, probes):
    x = jnp.transpose(joined, (0, 2, 3, 1, 4)).reshape(L, HB, 2, C, W)
    hbm = pl.BlockSpec(memory_space=pltpu.HBM)
    vmem = pl.BlockSpec(memory_space=pltpu.VMEM)
    dma = pltpu.SemaphoreType.DMA
    f32, bf16 = jnp.float32, jnp.bfloat16
    outs = (
        jax.ShapeDtypeStruct((L, ROWS, W), bf16),
        jax.ShapeDtypeStruct((L, ROWS, W), bf16),
        jax.ShapeDtypeStruct((L, TC, ROWS), bf16),
    )
    x = pltpu.with_memory_space_constraint(x, pltpu.HBM)
    probes = pltpu.with_memory_space_constraint(probes, pltpu.HBM)
    held = pl.pallas_call(
        exchange,
        out_shape=(jax.ShapeDtypeStruct((2 * L, TILES, ROWS + 8, LANES), f32), outs[2]),
        in_specs=[hbm, hbm],
        out_specs=(vmem, vmem),
        scratch_shapes=[
            pltpu.VMEM((J, C, W), bf16),
            pltpu.VMEM((L, T, W), bf16),
            pltpu.VMEM((TILES, J * PITCH, LANES), f32),
            pltpu.VMEM((C, J, W), bf16),
            pltpu.VMEM((R, J, W), bf16),
            pltpu.VMEM((TILES, J + 8, LANES), f32),
            pltpu.VMEM((L, NY, NX, TC, 2 * HALFW), f32),
            pltpu.VMEM((L, NY - 1, NX, TC, 2 * HALFW), f32),
            pltpu.VMEM((L, NX, TC, 2 * HALFW), f32),
            pltpu.VMEM((L, TC, 2 * HALFW), f32),
            pltpu.VMEM((2 * LANES, LANES), f32),
            pltpu.VMEM((NZ, 4, 4, LANES), bf16),
            pltpu.VMEM((NZ, 4, 4, LANES), bf16),
            pltpu.VMEM((4, NZ, 4, LANES), bf16),
            pltpu.VMEM((512, LANES), f32),
            dma((2 * L,)), dma,
            dma, dma((-(-(R - 1) // GROUP),)),
            dma, dma((L,)),
            dma((L,)), dma((L,)),
            dma, dma,
            dma, dma,
            pltpu.SemaphoreType.REGULAR, pltpu.SemaphoreType.REGULAR,
        ],
        compiler_params=pltpu.CompilerParams(
            collective_id=0, has_side_effects=True, vmem_limit_bytes=32 * 2**20
        ),
        name="exchange",
    )(x, probes)
    return pl.pallas_call(
        emit,
        out_shape=outs,
        in_specs=[vmem, vmem],
        out_specs=(hbm, hbm, hbm),
        scratch_shapes=[pltpu.VMEM((2 * L, ROWS, W), bf16), dma((2 * L * CUTS + 1,))],
        compiler_params=pltpu.CompilerParams(vmem_limit_bytes=4 * 2**20),
        name="emit",
    )(*held)


def solution(mesh):
    return jax.shard_map(
        body,
        mesh=mesh,
        in_specs=(P(None, None, "row", None, "col"), P(None, None, "col")),
        out_specs=(P(None, "row", "col"), P(None, "row", "col"), P(None, "col", "row")),
        check_vma=False,
    )
```

```python
import functools

import jax
import jax.numpy as jnp
from jax import lax
from jax.experimental import pallas as pl
from jax.experimental.pallas import tpu as pltpu
from jax.sharding import PartitionSpec as P

MESH = pl.DeviceIdType.MESH
L, C, R, B, W = 2, 32, 32, 28, 512
HB = B // 2
J = L * B
T = 128
NY, NX, NZ = 4, 2, 8
FIRST = (2, 14, 19, 31)
NEXT = (12, 29, 4, 21)
ORDER = FIRST + NEXT + tuple(n for n in (25 * s % 32 for s in range(1, 32)) if n not in FIRST + NEXT)
NEAR = 11
SENDNEAR = len(FIRST)
SENDNEXT = SENDNEAR + len(NEXT)
GROUP = 4
EARLY = 22
MIDWAY = 5
BEFORE = 6
HIDDEN = (4, 3, 5, 2, 6, 1, 7)
AHEAD = 2
CUTS = 2
LIMIT = 24
BONUS = (4, 3, 0, 0, 0, 0, 0, 0)
TC = T // (NY * NX)
PITCH = C + 1
LANES = 128
TILES = W // LANES
HALFW = 512
ROWS = C * HB


def plan(z, bonus):
    def rank(n):
        return n - (bonus[(z + ORDER[n] // 2) % NZ] if n >= LIMIT else 0)

    return [ORDER[n] + R * (n // GROUP) for n in sorted(range(R - 1), key=rank)]


def exchange(
    x_hbm, p_hbm, lined, hid, xs, pv, spread, msg, got, stage, part, in_a, summed, in_b, hidt, hsend, hmid, hgot, order,
    load_sem, p_sem, w_send, w_recv, a_send, a_recv, b_send, b_recv, h_send, h_recv, m_send, m_recv, near_sem, far_sem,
):
    me = lax.axis_index("row")
    col = lax.axis_index("col")
    xh, y = lax.div(col, NY), lax.rem(col, NY)
    xl, z, core = lax.div(me, 2 * NZ), lax.rem(lax.div(me, 2), NZ), lax.rem(me, 2)

    def moved(turn, sign):
        dx, dz, dc = lax.div(turn, 2 * NZ), lax.rem(lax.div(turn, 2), NZ), lax.rem(turn, 2)
        there = lax.rem(z + NZ + sign * dz, NZ)
        return lax.rem(xl + dx, 2) * (2 * NZ) + there * 2 + lax.rem(core + dc, 2)

    for q in range(2 * L):
        pltpu.make_async_copy(x_hbm.at[q % L, :, q // L], xs.at[pl.ds(q * HB, HB)], load_sem.at[q]).start()
    pltpu.make_async_copy(p_hbm, pv, p_sem).start()

    barrier = pltpu.get_barrier_semaphore()

    partner = (1 - xh) * NY + y
    for n in (n for n in ORDER if (n // 2 + 1) % NZ <= 2):
        pl.semaphore_signal(barrier, inc=1, device_id={"row": moved(n, 1)}, device_id_type=MESH)
    pl.semaphore_signal(barrier, inc=1, device_id={"col": partner}, device_id_type=MESH)
    for dy in range(1, NY):
        pl.semaphore_signal(barrier, inc=1, device_id={"col": xh * NY + lax.rem(y + dy, NY)}, device_id_type=MESH)

    for q in range(2 * L):
        pltpu.make_async_copy(x_hbm.at[q % L, :, q // L], xs.at[pl.ds(q * HB, HB)], load_sem.at[q]).wait()
        for i in range(HB):
            j = q * HB + i
            rows = xs[j].astype(jnp.float32)
            for c in range(TILES):
                spread[c, pl.ds(j * PITCH, C), :] = rows[:, c * LANES:(c + 1) * LANES]
    def build(k):
        for c in range(TILES):
            msg[k, :, pl.ds(c * LANES, LANES)] = spread[c, pl.ds(k, J, stride=PITCH), :].astype(jnp.bfloat16)

    plans = [plan(n, BONUS) for n in range(NZ)]

    def choice(n):
        options = [p[n] for p in plans]
        code = jnp.int32(options[0])
        for at, option in enumerate(options):
            if option != options[0]:
                code = jnp.where(z == at, jnp.int32(option), code)
        return moved(lax.rem(code, R), 1), lax.div(code, R)

    chosen = [choice(n) for n in range(R - 1)]

    def start_weights(n):
        to, which = chosen[n]
        pltpu.make_async_remote_copy(
            src_ref=msg.at[to], dst_ref=got.at[me], send_sem=w_send, recv_sem=w_recv.at[which],
            device_id={"row": to}, device_id_type=MESH,
        ).start()

    seat = xl * 2 + core

    def start_hidden(dz):
        there = lax.rem(z + dz, NZ)
        pltpu.make_async_remote_copy(
            src_ref=hsend.at[there], dst_ref=hmid.at[z], send_sem=h_send, recv_sem=h_recv,
            device_id={"row": moved(2 * dz, 1)}, device_id_type=MESH,
        ).start()

    def pass_hidden(turn):
        to = moved(turn, 1)
        other = lax.div(to, 2 * NZ) * 2 + lax.rem(to, 2)
        pltpu.make_async_remote_copy(
            src_ref=hmid.at[:, other], dst_ref=hgot.at[seat], send_sem=m_send, recv_sem=m_recv,
            device_id={"row": to}, device_id_type=MESH,
        ).start()

    def send(first, last):
        for n in range(first, last):
            if n + AHEAD < R - 1:
                build(chosen[n + AHEAD][0])
            start_weights(n)

    def tell(sem, steps):
        for turn in (2 * steps, 2 * (NZ - steps)):
            pl.semaphore_signal(sem, inc=1, device_id={"row": moved(turn, 1)}, device_id_type=MESH)

    for n in range(AHEAD):
        build(chosen[n][0])
    pl.semaphore_wait(barrier, NEAR + NY)
    for side, turn in enumerate((2, 2 * (NZ - 1))):
        pl.semaphore_signal(near_sem.at[side], inc=1, device_id={"row": moved(turn, 1)}, device_id_type=MESH)
    send(0, SENDNEAR)
    pl.semaphore_wait(near_sem.at[0], 1)
    send(SENDNEAR, SENDNEAR + 2)
    pl.semaphore_wait(near_sem.at[1], 1)
    tell(far_sem, 2)
    send(SENDNEAR + 2, SENDNEXT)
    pltpu.make_async_copy(p_hbm, pv, p_sem).wait()
    for l in range(L):
        for gu in range(2):
            rows = xs[pl.ds((gu * L + l) * HB, HB)].reshape(ROWS, W)
            proj = lax.dot_general(
                pv[l], rows, (((1,), (1,)), ((), ())), preferred_element_type=jnp.float32
            )
            for a in range(NX):
                for b in range(NY):
                    t = (a * NY + b) * TC
                    part[l, b, a, :, pl.ds(gu * HALFW, ROWS)] = proj[t:t + TC]
        for dy in range(1, NY):
            to = lax.rem(y + dy, NY)
            pltpu.make_async_remote_copy(
                src_ref=part.at[l, to], dst_ref=in_a.at[l, dy - 1], send_sem=a_send, recv_sem=a_recv.at[l],
                device_id={"col": xh * NY + to}, device_id_type=MESH,
            ).start()
    for n in range(EARLY + AHEAD, R - 1):
        build(chosen[n][0])
    build(me)
    pl.semaphore_wait(far_sem, 2)
    send(SENDNEXT, EARLY)

    def place(p, rows_of):
        for c in range(TILES):
            stage[c, pl.ds(0, J), :] = rows_of[p, :, pl.ds(c * LANES, LANES)].astype(jnp.float32)
        for c in range(TILES):
            for q in range(2 * L):
                lined[q, c, pl.ds(p * HB, HB), :] = stage[c, pl.ds(q * HB, HB), :]

    place(me, msg)

    phase_b = []
    for l in range(L):
        pltpu.make_async_copy(in_a.at[l], in_a.at[l], a_recv.at[l]).wait()
        summed[l] = part[l, y] + in_a[l, 0] + in_a[l, 1] + in_a[l, 2]
        phase_b.append(pltpu.make_async_remote_copy(
            src_ref=summed.at[l, 1 - xh], dst_ref=in_b.at[l], send_sem=b_send.at[l], recv_sem=b_recv.at[l],
            device_id={"col": partner}, device_id_type=MESH,
        ))
        phase_b[l].start()
    act = []
    for l in range(L):
        phase_b[l].wait_recv()
        total = summed[l, xh] + in_b[l]
        left, right = total[:, :HALFW], total[:, HALFW:]
        act.append(left / (1.0 + jnp.exp(-left)) * right)
    stacked = jnp.concatenate(
        [act[l][:, g * LANES:(g + 1) * LANES] for g in range(4) for l in range(L)], axis=0
    )
    hidt[pl.ds(0, LANES), :] = stacked.T
    for k in range(C):
        hsend[k // 2 % NZ, k // (2 * NZ) * 2 + k % 2] = hidt[pl.ds(k, 4, stride=C), :].astype(jnp.bfloat16)

    for dz in HIDDEN:
        start_hidden(dz)
    for n in range(EARLY, R - 1):
        start_weights(n)
    hmid[z] = hsend[z]

    def groups(first, last):
        for g in range(first, last):
            turns = ORDER[g * GROUP:(g + 1) * GROUP]
            many = pl.ds(0, len(turns))
            pltpu.make_async_copy(got.at[many], got.at[many], w_recv.at[g]).wait()

            def arrived(i, _):
                turn = jnp.int32(turns[0])
                for n, other in enumerate(turns[1:]):
                    turn = jnp.where(i > n, jnp.int32(other), turn)
                place(moved(turn, -1), got)
                return _

            lax.fori_loop(0, len(turns), arrived, 0)

    groups(0, MIDWAY)
    pltpu.make_async_copy(hmid.at[pl.ds(0, NZ - 1)], hmid.at[pl.ds(0, NZ - 1)], h_recv).wait()
    for turn in (1, 2 * NZ, 2 * NZ + 1):
        pass_hidden(turn)
    hgot[seat] = hmid[:, seat]
    groups(MIDWAY, BEFORE)
    pltpu.make_async_copy(hgot.at[pl.ds(0, 3)], hgot.at[pl.ds(0, 3)], m_recv).wait()
    for g in (3, 0, 1, 2):
        n = 2 if g == 3 else 4
        for p in range(R):
            piece = hgot[p // (2 * NZ) * 2 + p % 2, p // 2 % NZ].astype(jnp.float32)
            order[pl.ds(p * HB + 4 * g, n), :] = pltpu.roll(piece, (LANES - 32 * g) % LANES, 1)[:n]
    flat = order[...].T
    for l in range(L):
        hid[l] = flat[l * TC:(l + 1) * TC, :ROWS].astype(jnp.bfloat16)
    groups(BEFORE, -(-(R - 1) // GROUP))

    pltpu.make_async_copy(msg.at[pl.ds(0, R - 1)], msg.at[pl.ds(0, R - 1)], w_send).wait()
    pltpu.make_async_copy(in_a, in_a, a_send).wait()
    for copy in phase_b:
        copy.wait_send()
    pltpu.make_async_copy(hmid.at[pl.ds(0, NZ - 1)], hmid.at[pl.ds(0, NZ - 1)], h_send).wait()
    pltpu.make_async_copy(hgot.at[pl.ds(0, 3)], hgot.at[pl.ds(0, 3)], m_send).wait()


def emit(lined, hid_in, gate, up, hid, rows, sems):
    copies = [pltpu.make_async_copy(hid_in, hid, sems.at[2 * L * CUTS])]
    copies[0].start()
    for q in range(2 * L):
        for n in range(CUTS):
            span = pl.ds(n * (ROWS // CUTS), ROWS // CUTS)
            for c in range(TILES):
                rows[q, span, pl.ds(c * LANES, LANES)] = lined[q, c, span].astype(jnp.bfloat16)
            copies.append(pltpu.make_async_copy(
                rows.at[q, span], (gate, up)[q // L].at[q % L, span], sems.at[q * CUTS + n]
            ))
            copies[-1].start()
    for copy in copies:
        copy.wait()


def body(joined, probes):
    x = jnp.transpose(joined, (0, 2, 3, 1, 4)).reshape(L, HB, 2, C, W)
    hbm = pl.BlockSpec(memory_space=pltpu.HBM)
    vmem = pl.BlockSpec(memory_space=pltpu.VMEM)
    dma = pltpu.SemaphoreType.DMA
    f32, bf16 = jnp.float32, jnp.bfloat16
    outs = (
        jax.ShapeDtypeStruct((L, ROWS, W), bf16),
        jax.ShapeDtypeStruct((L, ROWS, W), bf16),
        jax.ShapeDtypeStruct((L, TC, ROWS), bf16),
    )
    x = pltpu.with_memory_space_constraint(x, pltpu.HBM)
    probes = pltpu.with_memory_space_constraint(probes, pltpu.HBM)
    held = pl.pallas_call(
        exchange,
        out_shape=(jax.ShapeDtypeStruct((2 * L, TILES, ROWS + 8, LANES), f32), outs[2]),
        in_specs=[hbm, hbm],
        out_specs=(vmem, vmem),
        scratch_shapes=[
            pltpu.VMEM((J, C, W), bf16),
            pltpu.VMEM((L, T, W), bf16),
            pltpu.VMEM((TILES, J * PITCH, LANES), f32),
            pltpu.VMEM((C, J, W), bf16),
            pltpu.VMEM((R, J, W), bf16),
            pltpu.VMEM((TILES, J + 8, LANES), f32),
            pltpu.VMEM((L, NY, NX, TC, 2 * HALFW), f32),
            pltpu.VMEM((L, NY - 1, NX, TC, 2 * HALFW), f32),
            pltpu.VMEM((L, NX, TC, 2 * HALFW), f32),
            pltpu.VMEM((L, TC, 2 * HALFW), f32),
            pltpu.VMEM((2 * LANES, LANES), f32),
            pltpu.VMEM((NZ, 4, 4, LANES), bf16),
            pltpu.VMEM((NZ, 4, 4, LANES), bf16),
            pltpu.VMEM((4, NZ, 4, LANES), bf16),
            pltpu.VMEM((512, LANES), f32),
            dma((2 * L,)), dma,
            dma, dma((-(-(R - 1) // GROUP),)),
            dma, dma((L,)),
            dma((L,)), dma((L,)),
            dma, dma,
            dma, dma,
            pltpu.SemaphoreType.REGULAR((2,)), pltpu.SemaphoreType.REGULAR,
        ],
        compiler_params=pltpu.CompilerParams(
            collective_id=0, has_side_effects=True, vmem_limit_bytes=32 * 2**20
        ),
        name="exchange",
    )(x, probes)
    return pl.pallas_call(
        emit,
        out_shape=outs,
        in_specs=[vmem, vmem],
        out_specs=(hbm, hbm, hbm),
        scratch_shapes=[pltpu.VMEM((2 * L, ROWS, W), bf16), dma((2 * L * CUTS + 1,))],
        compiler_params=pltpu.CompilerParams(vmem_limit_bytes=4 * 2**20),
        name="emit",
    )(*held)


def solution(mesh):
    return jax.shard_map(
        body,
        mesh=mesh,
        in_specs=(P(None, None, "row", None, "col"), P(None, None, "col")),
        out_specs=(P(None, "row", "col"), P(None, "row", "col"), P(None, "col", "row")),
        check_vma=False,
    )
```
